32 devices in a mesh: groups: 1, slab: 8 (over z, y), coil: 2 (over x), row: 2 (over core).
Axes of the slice: x: 2, y: 2, z: 4, core: 2. Of those that a mesh axis runs over, the one named last changes fastest.
Arguments:
- image: float32 [2, 128, 256, 128], P('groups', None, ('slab', 'row')), may hold values from -6 to 6
- sens: bfloat16 [2, 16, 128, 256, 128], P('groups', 'coil', None, ('slab', 'row')), may hold values from -1.5 to 1.5
- measured: bfloat16 [2, 16, 128, 256, 128], P('groups', 'coil', ('slab', 'row')), may hold values from -3 to 3
- mask: int32 [128, 256], P(('slab', 'row')), may hold values from 0 to 1, as said below
- thresholds: float32 [2, 7], replicated, may hold values from 0.1 to 1.5
Outputs:
- image_next: float32 [2, 128, 256, 128], P('groups', None, ('slab', 'row'))
The draws below stay inside these ranges and needn't reach their ends.
Inputs may be any that keep to these rules, and one draw needn't show every extreme that they name: `mask`: A calibration block of the 8 central phase-encode lines (ky from 60 to 67) is sampled at every kz; outside it each (ky, kz) is sampled independently at random.
All inputs are finite; a program needn't handle non-finite values.
Results may differ from the reference program's by a relative error of at most 0.013.
Values may be sent and summed in bfloat16 or wider, within the bound.
A program may use at most 128 MiB of HBM per device.

```python
import math
import jax
import jax.numpy as jnp
from jax import lax

X = 128
Y = 128
Z = 256
C = 16
LEVELS = 2


def draw_mask(key, part):
    drawn = jax.random.randint(key, (Y, Z), 0, 3)
    scattered = (drawn == 0).astype(jnp.int32)
    line_index = jnp.arange(Y, dtype=jnp.int32)[:, None]
    calibration = ((line_index >= Y // 2 - 4) & (line_index < Y // 2 + 4)).astype(jnp.int32)
    return jnp.maximum(scattered, jnp.broadcast_to(calibration, (Y, Z)))


def steps_of(key, extent, split, least, top_value):
    gain = 1.0
    for position, blocks in split:
        steps = jax.random.uniform(jax.random.fold_in(jax.random.fold_in(key, 6), position), (blocks,), jnp.float32, least / len(split), top_value / len(split))
        gain = gain * jnp.repeat(jnp.exp(steps), extent[position] // blocks).reshape((-1,) + (1,) * (len(extent) - 1 - position))
    return gain


def noise(stream_key, extent, width, bound, cuts=(), kind=jnp.bfloat16):
    result = width * jax.random.normal(stream_key, extent, jnp.float32)
    if cuts:
        result = result * steps_of(stream_key, extent, cuts, -0.22, 0.18)
    return jnp.clip(result, -bound, bound).astype(kind)


def setup_inputs(seed: int = 0, part: int = 0) -> dict:
    seeds = jax.random.split(jax.random.key(seed), 6)
    own_keys = jax.random.split(jax.random.fold_in(seeds[5], part), 6)
    image = noise(own_keys[0], (2, Y, Z, X), 1.0, 6.0, ((2, 16),), jnp.float32)
    sens = noise(own_keys[1], (2, C, Y, Z, X), 0.25, 1.5, ((1, 2), (3, 16)))
    measured = noise(own_keys[2], (2, C, Y, Z, X), 0.5, 3.0, ((1, 2), (2, 16)))
    mask = draw_mask(jax.random.fold_in(seeds[5], 71), part)
    thresholds = jnp.clip(jnp.exp(jax.random.uniform(seeds[4], (LEVELS, 7), jnp.float32, math.log(0.1), math.log(1.5))), 0.1, 1.5)
    return {"image": image, "sens": sens, "measured": measured, "mask": mask, "thresholds": thresholds}


half_root = 0.7071067811865476
quarter_root = 0.3535533905932738
step_size = 0.5

def fourier_table(length, sign):
    index = jnp.arange(length, dtype=jnp.int32)
    phase = index[:, None] * index[None, :] % length
    theta = phase.astype(jnp.float32) * jnp.float32(2.0 * math.pi / length)
    scale = jnp.float32(1.0 / math.sqrt(length))
    real = jnp.cos(theta) * scale
    imaginary = jnp.sin(theta) * (sign * scale)
    upper = jnp.stack([real, -imaginary])
    lower = jnp.stack([imaginary, real])
    return jnp.stack([upper, lower]).astype(jnp.bfloat16)

def contract(form, values, table):
    return jnp.einsum(form, values.astype(jnp.float32), table.astype(jnp.float32), precision=lax.Precision.HIGHEST)

def complex_product(left, right):
    return jnp.stack([left[0] * right[0] - left[1] * right[1], left[0] * right[1] + left[1] * right[0]])

def roll_after(values, along, offset):
    return jnp.roll(values, -offset, axis=along)

def roll_before(values, along, offset):
    return jnp.roll(values, offset, axis=along)

def split_bands(bands, along, offset, after):
    moved = after(bands, along, offset)
    return jnp.concatenate([(bands + moved) * half_root, (bands - moved) * half_root], axis=0)

def merge_bands(bands, along, offset, before):
    half = bands.shape[0] // 2
    lower = bands[:half]
    upper = bands[half:]
    return (lower + upper + before(lower - upper, along, offset)) * quarter_root

def shrink_detail(detail, limit):
    magnitude = jnp.sqrt(detail[:, 0] * detail[:, 0] + detail[:, 1] * detail[:, 1])
    limit = limit.reshape((-1, 1, 1, 1))
    factor = jnp.maximum(magnitude - limit, 0.0) / jnp.maximum(magnitude, limit)
    return detail * factor[:, None]

def wavelet_shrink(descent, thresholds, moves):
    coarse = descent[None]
    details = []
    for level in range(thresholds.shape[0]):
        offset = 2 ** level
        bands = coarse
        for along, after, before in moves:
            bands = split_bands(bands, along, offset, after)
        coarse = bands[:1]
        details.append(shrink_detail(bands[1:], thresholds[level]))
    for level in reversed(range(thresholds.shape[0])):
        offset = 2 ** level
        bands = jnp.concatenate([coarse, details[level]], axis=0)
        for along, after, before in reversed(moves):
            bands = merge_bands(bands, along, offset, before)
        coarse = bands
    return coarse[0]

def reference(image, sens, measured, mask, thresholds):
    table_readout = fourier_table(image.shape[3], -1.0)
    table_phase = fourier_table(image.shape[1], -1.0)
    table_depth = fourier_table(image.shape[2], -1.0)
    inverse_readout = fourier_table(image.shape[3], 1.0)
    inverse_phase = fourier_table(image.shape[1], 1.0)
    inverse_depth = fourier_table(image.shape[2], 1.0)
    sampled = mask.astype(jnp.float32)[None, :, :, None]

    def coil_step(total, pieces):
        coil_sens, coil_data = pieces
        sens_wide = coil_sens.astype(jnp.float32)
        coil_image = complex_product(sens_wide, image).astype(jnp.bfloat16)
        readout_done = contract('tyzj,stjk->syzk', coil_image, table_readout).astype(jnp.bfloat16)
        phase_done = contract('tjzx,stjk->skzx', readout_done, table_phase).astype(jnp.bfloat16)
        spectrum = contract('tyjx,stjk->sykx', phase_done, table_depth)
        residual = (sampled * (spectrum - coil_data.astype(jnp.float32))).astype(jnp.bfloat16)
        depth_back = contract('tyjx,stjk->sykx', residual, inverse_depth).astype(jnp.bfloat16)
        phase_back = contract('tjzx,stjk->skzx', depth_back, inverse_phase).astype(jnp.bfloat16)
        readout_back = contract('tyzj,stjk->syzk', phase_back, inverse_readout)
        term = jnp.stack([sens_wide[0] * readout_back[0] + sens_wide[1] * readout_back[1], sens_wide[0] * readout_back[1] - sens_wide[1] * readout_back[0]])
        return (total + term, None)
    gradient, _ = lax.scan(coil_step, jnp.zeros(image.shape, jnp.float32), (jnp.moveaxis(sens, 1, 0), jnp.moveaxis(measured, 1, 0)))
    descent = image - step_size * gradient
    moves = [(4, roll_after, roll_before), (2, roll_after, roll_before), (3, roll_after, roll_before)]
    return wavelet_shrink(descent, thresholds, moves)
```

```python
import functools
import math

import jax
import jax.numpy as jnp
import ml_dtypes
import numpy as np
from jax import lax
from jax.experimental import pallas as pl
from jax.experimental.pallas import tpu as pltpu
from jax.sharding import PartitionSpec as P

MESH = pl.DeviceIdType.MESH
half_root = 0.7071067811865476
quarter_root = 0.3535533905932738
step_size = 0.5
CALIBRATION = 8
LATE_COILS = 2


def fourier_table(length, sign):
    index = np.arange(length)
    theta = (index[:, None] * index[None, :] % length) * (2.0 * math.pi / length)
    real = np.cos(theta) / math.sqrt(length)
    imaginary = sign * np.sin(theta) / math.sqrt(length)
    return np.stack([np.stack([real, -imaginary]), np.stack([imaginary, real])])


def split_plane(plane, offset):
    cells_y, cells_x = plane.shape
    moved = pltpu.roll(plane, cells_x - offset, 1)
    bands = []
    for part in (plane + moved, plane - moved):
        bands.append((part, pltpu.roll(part, cells_y - offset, 0)))
    (low, low_moved), (high, high_moved) = bands
    return [low + low_moved, high + high_moved, low - low_moved, high - high_moved]


def merge_plane(bands, offset):
    across = []
    for lower, upper in ((bands[0], bands[2]), (bands[1], bands[3])):
        across.append(lower + upper + pltpu.roll(lower - upper, offset, 0))
    lower, upper = across
    return lower + upper + pltpu.roll(lower - upper, offset, 1)


def shrink_pair(real, imaginary, limit):
    factor = jnp.maximum(1.0 - limit * lax.rsqrt(real * real + imaginary * imaginary), 0.0)
    return real * factor, imaginary * factor


def wavelet_kernel(levels, planes, limits, source, result, *scratch):
    halo = 2**levels - 1
    stop = halo + planes
    coarse_refs = (source,) + scratch[: levels - 1]
    merged_refs = (None,) + scratch[levels - 1 : 2 * (levels - 1)]
    split_ref, carry_ref = scratch[2 * (levels - 1) :]
    extent = planes + 2 * halo
    for level in range(levels - 1):
        offset = 2**level
        extent -= offset
        finer, coarser = coarse_refs[level], coarse_refs[level + 1]

        def coarsen(n, _, offset=offset, finer=finer, coarser=coarser):
            for t in range(2):
                total = finer[t, n] + finer[t, n + offset]
                total = total + pltpu.roll(total, total.shape[1] - offset, 1)
                total = total + pltpu.roll(total, total.shape[0] - offset, 0)
                coarser[t, n] = total * half_root**3
            return 0

        lax.fori_loop(0, extent, coarsen, 0)
    for level in reversed(range(levels)):
        offset = 2**level
        slots = offset + 1
        first = halo - (offset - 1)
        start = first - offset
        coarse = coarse_refs[level]

        def enter(n, _, offset=offset, coarse=coarse, slots=slots):
            for t in range(2):
                for b, band in enumerate(split_plane(coarse[t, n] * half_root**3, offset)):
                    split_ref[lax.rem(n, slots), b, t] = band
            return 0

        lax.fori_loop(start, start + offset, enter, 0)

        def advance(n, _, level=level, offset=offset, slots=slots, first=first, enter=enter):
            enter(n + offset, 0)
            here, there, back = lax.rem(n, slots), lax.rem(n + offset, slots), lax.rem(n, offset)
            merged = [[], []]
            for b in range(4):
                near = [split_ref[here, b, t] for t in range(2)]
                far = [split_ref[there, b, t] for t in range(2)]
                high = shrink_pair(near[0] - far[0], near[1] - far[1], limits[level, b + 3])
                if b:
                    low = shrink_pair(near[0] + far[0], near[1] + far[1], limits[level, b - 1])
                elif level < levels - 1:
                    low = [merged_refs[level + 1][t, n] for t in range(2)]
                else:
                    low = (near[0] + far[0], near[1] + far[1])
                for t in range(2):
                    merged[t].append(low[t] + high[t] + carry_ref[back, b, t])
                    carry_ref[back, b, t] = low[t] - high[t]

            @pl.when(n >= first)
            def _():
                for t in range(2):
                    value = merge_plane(merged[t], offset) * quarter_root**3
                    if level:
                        merged_refs[level][t, n] = value
                    else:
                        result[t, n - halo] = value

            return 0

        lax.fori_loop(start, stop, advance, 0)


def wavelet_shrink(source, thresholds, planes):
    levels = thresholds.shape[0]
    halo = 2**levels - 1
    parts, _, cells_y, cells_x = source.shape
    plane = (cells_y, cells_x)
    store = [pltpu.VMEM((parts, planes + 2 * halo) + plane, jnp.float32)] * (2 * (levels - 1))
    whole = pl.BlockSpec(memory_space=pltpu.VMEM)
    return pl.pallas_call(
        functools.partial(wavelet_kernel, levels, planes),
        out_shape=jax.ShapeDtypeStruct((parts, planes) + plane, jnp.float32),
        in_specs=[pl.BlockSpec(memory_space=pltpu.SMEM), whole],
        out_specs=whole,
        scratch_shapes=store
        + [
            pltpu.VMEM((2 ** (levels - 1) + 1, 4, parts) + plane, jnp.float32),
            pltpu.VMEM((2 ** (levels - 1), 4, parts) + plane, jnp.float32),
        ],
        compiler_params=pltpu.CompilerParams(vmem_limit_bytes=32 * 2**20),
        name="wavelet",
    )(thresholds, source)


class Sizes:
    def __init__(self, image, sens, measured, thresholds, shards, coil_groups):
        self.shards, self.coil_groups = shards, coil_groups
        _, self.y, self.planes, self.x = image.shape
        self.z = measured.shape[3]
        self.coils = sens.shape[1]
        self.lines = self.y // shards
        self.part_lines = min(self.lines, 4)
        self.parts = self.lines // self.part_lines
        self.group = min(self.planes, 4)
        self.groups = self.planes // self.group
        self.halo = 2 ** thresholds.shape[0] - 1
        self.late = min(LATE_COILS, self.coils)
        self.early = self.coils - self.late
        first = self.y // 2 - CALIBRATION // 2
        self.calibration = (first, first + CALIBRATION)
        self.skipped = [
            [d for d in range(shards) if self.inside(d, h)] for h in range(self.parts)
        ]

    def inside(self, shard, part):
        start = shard * self.lines + part * self.part_lines
        return self.calibration[0] <= start and start + self.part_lines <= self.calibration[1]

    def is_skipped(self, shard, part):
        found = shard < 0
        for d in self.skipped[part]:
            found = found | (shard == d)
        return found


def tables(sizes):
    n, y, z, planes = sizes.shards, sizes.y, sizes.z, sizes.planes
    phase = fourier_table(y, -1.0)
    phase_rows = phase.reshape(2, 2, y, n, sizes.parts, sizes.part_lines)
    phase_rows = phase_rows.transpose(3, 4, 0, 5, 1, 2).reshape(2 * y, 2 * y)
    inverse = fourier_table(y, 1.0)
    inverse_rows = inverse.transpose(0, 3, 1, 2).reshape(2 * y, 2 * y)
    kept = np.zeros((y,))
    for h in range(sizes.parts):
        for d in sizes.skipped[h]:
            start = d * sizes.lines + h * sizes.part_lines
            kept[start : start + sizes.part_lines] = 1.0
    central = inverse * kept[None, None, :, None]
    central = central.reshape(2, 2, n, sizes.parts, sizes.part_lines, y)
    central = central.transpose(0, 5, 2, 3, 1, 4).reshape(2 * y, 2 * y)
    depth = fourier_table(z, -1.0).transpose(0, 3, 1, 2).reshape(2 * z, 2 * z)
    back = fourier_table(z, 1.0).reshape(2, 2, z, n, sizes.groups, sizes.group)
    back = back.transpose(3, 4, 0, 5, 1, 2).reshape(2 * z, 2 * z)
    readout = fourier_table(sizes.x, 1.0).transpose(1, 2, 0, 3).reshape(2 * sizes.x, 2 * sizes.x)
    found = (phase_rows, central, depth, back, inverse_rows, readout)
    return [jnp.asarray(t.astype(np.float32).astype(ml_dtypes.bfloat16)) for t in found]


def dot(left, right):
    return jnp.dot(left, right, preferred_element_type=jnp.float32)


def gradient_kernel(
    sizes, image, sens, measured, sampled, phase, central, depth, back, inverse, readout, source,
    out_f, in_f, out_b, in_b, sens_kept, wide, sens_slots, measured_slots, totals, edge_out, edge_in,
    sens_sem, measured_sem, out_f_sem, in_f_sem, out_b_sem, in_b_sem, out_q_sem, in_q_sem,
    total_out_sem, total_in_sem, edge_out_sem, edge_in_sem,
):
    n, x = sizes.shards, sizes.x
    coils, early, late = sizes.coils, sizes.early, sizes.late
    planes, halo, pair = sizes.planes, sizes.halo, 2
    rows_f = 2 * sizes.part_lines
    rows_b = 2 * sizes.group
    cells = sizes.y * planes
    rows_n = lax.axis_size("row")
    here = lax.axis_index("slab") * rows_n + lax.axis_index("row")
    scan, coil_here = lax.axis_index("groups"), lax.axis_index("coil")

    def device(shard, coil=None):
        return (scan, shard // rows_n, coil_here if coil is None else coil, lax.rem(shard, rows_n))

    def remote(src, dst, sent, got, target):
        return pltpu.make_async_remote_copy(
            src_ref=src, dst_ref=dst, send_sem=sent, recv_sem=got, device_id=target, device_id_type=MESH
        )

    def arrived(ref, sem):
        pltpu.make_async_copy(ref, ref, sem).wait()

    def sens_copy(c):
        slot = lax.rem(c, 2)
        return pltpu.make_async_copy(sens.at[:, c], sens_slots.at[slot], sens_sem.at[slot])

    def measured_copy(c):
        slot = lax.rem(c, 2)
        return pltpu.make_async_copy(measured.at[:, c], measured_slots.at[slot], measured_sem.at[slot])

    sens_copy(0).start()

    def forward(c, _):
        slot = lax.rem(c, 2)

        @pl.when(c + 1 < coils)
        def _():
            sens_copy(c + 1).start()

        sens_copy(c).wait()
        block = cells // 16

        def widen(i, _):
            at = pl.multiple_of(i * block, block)
            for t in range(2):
                wide[pl.ds(t * cells + at, block), :] = sens_slots[slot, t, pl.ds(at, block), :].astype(jnp.float32)
            return 0

        lax.fori_loop(0, 16, widen, 0)

        def plane(p, _):
            sr, si = (wide[pl.ds(t * cells + p, sizes.y, stride=planes), :] for t in range(2))
            ur, ui = (image[t, pl.ds(p, sizes.y, stride=planes), :] for t in range(2))
            sens_kept[c, 0, p] = sr.astype(jnp.bfloat16)
            sens_kept[c, 1, p] = si.astype(jnp.bfloat16)
            coil_image = jnp.concatenate([sr * ur - si * ui, sr * ui + si * ur], axis=0).astype(jnp.bfloat16)
            done = dot(phase[...], coil_image).reshape(n, sizes.parts, rows_f, x)
            out_f[c, :, :, p] = done.astype(jnp.bfloat16)
            return 0

        lax.fori_loop(0, planes, plane, 0)

        def send(d, _):
            to = lax.rem(here + d, n)
            for h in range(sizes.parts):

                @pl.when(jnp.logical_not(sizes.is_skipped(to, h)))
                def _():
                    remote(out_f.at[c, to, h], in_f.at[c, here, h], out_f_sem.at[c, h], in_f_sem.at[c, h], device(to)).start()

            return 0

        lax.fori_loop(1, n, send, 0)
        for h in range(sizes.parts):
            in_f[c, here, h] = out_f[c, here, h]

        def middle(p, _):
            lines = out_f[c, :, :, p].astype(jnp.float32).reshape(2 * sizes.y, x).astype(jnp.bfloat16)
            value = dot(central[...], lines)
            add_gradient(c, p, value[: sizes.y], value[sizes.y :], c == 0)
            return 0

        lax.fori_loop(0, planes, middle, 0)
        return 0

    def add_gradient(c, p, real, imaginary, fresh=None):
        sr = sens_kept[c, 0, p].astype(jnp.float32)
        si = sens_kept[c, 1, p].astype(jnp.float32)
        for t, term in ((0, sr * real + si * imaginary), (1, sr * imaginary - si * real)):
            held = source[t, halo + p]
            if fresh is not None:
                held = jnp.where(fresh, jnp.zeros_like(held), held)
            source[t, halo + p] = held + term

    lax.fori_loop(0, coils, forward, 0)

    measured_copy(0).start()

    def lines_of(c, _):
        slot = lax.rem(c, 2)

        @pl.when(c + 1 < coils)
        def _():
            measured_copy(c + 1).start()

        measured_copy(c).wait()
        for h in range(sizes.parts):
            skipped = sizes.is_skipped(here, h)

            @pl.when(jnp.logical_not(skipped))
            def _():
                arrived(in_f.at[c, pl.ds(0, n - 1), h], in_f_sem.at[c, h])

                def widen(i, _):
                    rows = planes * rows_f
                    at = pl.multiple_of(i * rows, rows)
                    wide[pl.ds(at, rows), :] = in_f[c, i, h].astype(jnp.float32).reshape(rows, x)
                    return 0

                lax.fori_loop(0, n, widen, 0)

            @pl.when(skipped)
            def _():
                def clear(i, _):
                    rows = planes * rows_f
                    wide[pl.ds(pl.multiple_of(i * rows, rows), rows), :] = jnp.zeros((rows, x), jnp.float32)
                    return 0

                lax.fori_loop(0, n, clear, 0)

            def two_lines(i, _):
                across = []
                for j in range(pair):
                    row = i * pair + j
                    parts = [wide[pl.ds(t * sizes.part_lines + row, sizes.z, stride=rows_f), :] for t in range(2)]
                    across.append(jnp.concatenate(parts, axis=0).astype(jnp.bfloat16))
                spectrum = dot(depth[...], jnp.concatenate(across, axis=1))
                residuals = []
                for j in range(pair):
                    line = h * sizes.part_lines + i * pair + j
                    both = jnp.concatenate([measured_slots[slot, t, line] for t in range(2)], axis=1)
                    data = dot(both, readout[...])
                    keep = sampled[line]
                    columns = slice(j * x, (j + 1) * x)
                    residuals.append(
                        jnp.concatenate(
                            [
                                keep * (spectrum[: sizes.z, columns] - data[:, :x]),
                                keep * (spectrum[sizes.z :, columns] - data[:, x:]),
                            ],
                            axis=0,
                        ).astype(jnp.bfloat16)
                    )
                returned = dot(back[...], jnp.concatenate(residuals, axis=1))
                for j in range(pair):
                    line = h * sizes.part_lines + i * pair + j
                    value = returned[:, j * x : (j + 1) * x].reshape(n, sizes.groups, rows_b, x)
                    out_b[c, :, :, line] = value.astype(jnp.bfloat16)
                return 0

            lax.fori_loop(0, sizes.part_lines // pair, two_lines, 0)

        in_b[c, here] = out_b[c, here]

        @pl.when(c < early)
        def _():
            def send(d, _):
                to = lax.rem(here + d, n)
                remote(out_b.at[c, to], in_b.at[c, here], out_b_sem.at[c], in_b_sem.at[c], device(to)).start()
                return 0

            lax.fori_loop(1, n, send, 0)

        return 0

    lax.fori_loop(0, coils, lines_of, 0)
    order = [0] + ([sizes.groups - 1] if sizes.groups > 1 else []) + list(range(1, sizes.groups - 1))
    last = pl.ds(early, late)
    for q in order:

        def send(d, _, q=q):
            to = lax.rem(here + d, n)
            remote(out_b.at[last, to, q], in_b.at[last, here, q], out_q_sem.at[q], in_q_sem.at[q], device(to)).start()
            return 0

        lax.fori_loop(1, n, send, 0)

    def combine(c, q):
        rows = sizes.lines * rows_b

        def widen(i, _):
            at = pl.multiple_of(i * rows, rows)
            wide[pl.ds(at, rows), :] = in_b[c, i, q].astype(jnp.float32).reshape(rows, x)
            return 0

        lax.fori_loop(0, n, widen, 0)

        def two_planes(i, _):
            across = []
            for j in range(pair):
                row = i * pair + j
                parts = [wide[pl.ds(t * sizes.group + row, sizes.y, stride=rows_b), :] for t in range(2)]
                across.append(jnp.concatenate(parts, axis=0).astype(jnp.bfloat16))
            value = dot(inverse[...], jnp.concatenate(across, axis=1))
            for j in range(pair):
                columns = slice(j * x, (j + 1) * x)
                add_gradient(c, q * sizes.group + i * pair + j, value[: sizes.y, columns], value[sizes.y :, columns])
            return 0

        lax.fori_loop(0, sizes.group // pair, two_planes, 0)

    def early_coil(c, _):
        arrived(in_b.at[c, pl.ds(0, n - 1)], in_b_sem.at[c])

        def each(q, _):
            combine(c, q)
            return 0

        lax.fori_loop(0, sizes.groups, each, 0)
        return 0

    lax.fori_loop(0, early, early_coil, 0)

    def total_copy(q, distance):
        to = lax.rem(coil_here + distance, sizes.coil_groups)
        return remote(
            totals.at[coil_here, q], totals.at[coil_here, q], total_out_sem.at[q, distance - 1],
            total_in_sem.at[q, distance - 1], device(here, to),
        )

    def finish(q):
        for distance in range(1, sizes.coil_groups):
            total_copy(q, distance).wait_recv()

        def plane(i, _):
            p = q * sizes.group + i
            for t in range(2):
                total = totals[0, q, t, i].astype(jnp.float32)
                for k in range(1, sizes.coil_groups):
                    total = total + totals[k, q, t, i].astype(jnp.float32)
                source[t, halo + p] = image[t, pl.ds(p, sizes.y, stride=planes), :] - step_size * total
            return 0

        lax.fori_loop(0, sizes.group, plane, 0)

    def edge_copy(side):
        to = lax.rem(here + (1, n - 1)[side], n)
        return remote(edge_out.at[side], edge_in.at[side], edge_out_sem.at[side], edge_in_sem.at[side], device(to))

    ends = set(order[:2])
    for step, q in enumerate(order):
        arrived(in_b.at[last, pl.ds(0, n - 1), q], in_q_sem.at[q])

        def each(c, _, q=q):
            combine(early + c, q)
            return 0

        lax.fori_loop(0, late, each, 0)
        for t in range(2):
            for i in range(sizes.group):
                totals[coil_here, q, t, i] = source[t, halo + q * sizes.group + i].astype(jnp.bfloat16)
        for distance in range(1, sizes.coil_groups):
            total_copy(q, distance).start()
        done = order[:step] if step else []
        if done:
            finish(done[-1])
        if ends.issubset(done) and not ends.issubset(done[:-1]):
            exchange_edges = True
        else:
            exchange_edges = False
        if exchange_edges:
            for t in range(2):
                edge_out[0, t] = source[t, planes : planes + halo].astype(jnp.bfloat16)
                edge_out[1, t] = source[t, halo : 2 * halo].astype(jnp.bfloat16)
            for side in range(2):
                edge_copy(side).start()
    finish(order[-1])
    if not ends.issubset(order[:-1]):
        for t in range(2):
            edge_out[0, t] = source[t, planes : planes + halo].astype(jnp.bfloat16)
            edge_out[1, t] = source[t, halo : 2 * halo].astype(jnp.bfloat16)
        for side in range(2):
            edge_copy(side).start()
    for side in range(2):
        edge_copy(side).wait_recv()
    for t in range(2):
        source[t, :halo] = edge_in[0, t].astype(jnp.float32)
        source[t, halo + planes :] = edge_in[1, t].astype(jnp.float32)

    for side in range(2):
        edge_copy(side).wait_send()
    for q in order:
        arrived(out_b.at[last, pl.ds(0, n - 1), q], out_q_sem.at[q])
        for distance in range(1, sizes.coil_groups):
            total_copy(q, distance).wait_send()

    def left(c, _):
        for h in range(sizes.parts):
            skipped = sizes.is_skipped(here, h)
            others = n - len(sizes.skipped[h])

            @pl.when(skipped)
            def _():
                arrived(out_f.at[c, pl.ds(0, others), h], out_f_sem.at[c, h])

            @pl.when(jnp.logical_not(skipped))
            def _():
                arrived(out_f.at[c, pl.ds(0, others - 1), h], out_f_sem.at[c, h])

        @pl.when(c < early)
        def _():
            arrived(out_b.at[c, pl.ds(0, n - 1)], out_b_sem.at[c])

        return 0

    lax.fori_loop(0, coils, left, 0)


def descent_planes(image, sens, measured, mask, thresholds):
    sizes = Sizes(image, sens, measured, thresholds, lax.axis_size(("slab", "row")), lax.axis_size("coil"))
    n, x, y, planes, coils = sizes.shards, sizes.x, sizes.y, sizes.planes, sizes.coils
    cells = y * planes
    sampled = jnp.broadcast_to(mask.astype(jnp.float32)[:, :, None], mask.shape + (x,))
    forward = (coils, n, sizes.parts, planes, 2 * sizes.part_lines, x)
    backward = (coils, n, sizes.groups, sizes.lines, 2 * sizes.group, x)
    bf, dma = jnp.bfloat16, pltpu.SemaphoreType.DMA
    rows = max(2 * cells, n * planes * 2 * sizes.part_lines, y * 2 * sizes.group)
    whole, anywhere = pl.BlockSpec(memory_space=pltpu.VMEM), pl.BlockSpec(memory_space=pl.ANY)
    others = max(sizes.coil_groups - 1, 1)
    return pl.pallas_call(
        functools.partial(gradient_kernel, sizes),
        out_shape=jax.ShapeDtypeStruct((2, planes + 2 * sizes.halo, y, x), jnp.float32),
        in_specs=[whole, anywhere, anywhere] + [whole] * 7,
        out_specs=whole,
        scratch_shapes=[
            pltpu.VMEM(forward, bf),
            pltpu.VMEM(forward, bf),
            pltpu.VMEM(backward, bf),
            pltpu.VMEM(backward, bf),
            pltpu.VMEM((coils, 2, planes, y, x), bf),
            pltpu.VMEM((rows, x), jnp.float32),
            pltpu.VMEM((2, 2, cells, x), bf),
            pltpu.VMEM((2, 2, sizes.lines, sizes.z, x), bf),
            pltpu.VMEM((sizes.coil_groups, sizes.groups, 2, sizes.group, y, x), bf),
            pltpu.VMEM((2, 2, sizes.halo, y, x), bf),
            pltpu.VMEM((2, 2, sizes.halo, y, x), bf),
            dma((2,)),
            dma((2,)),
            dma((coils, sizes.parts)),
            dma((coils, sizes.parts)),
            dma((coils,)),
            dma((coils,)),
            dma((sizes.groups,)),
            dma((sizes.groups,)),
            dma((sizes.groups, others)),
            dma((sizes.groups, others)),
            dma((2,)),
            dma((2,)),
        ],
        compiler_params=pltpu.CompilerParams(has_side_effects=True, vmem_limit_bytes=67043328),
        name="gradient",
    )(image.reshape(2, cells, x), sens.reshape(2, coils, cells, x), measured, sampled, *tables(sizes))


def shrinkage_step(image, sens, measured, mask, thresholds):
    source = descent_planes(image, sens, measured, mask, thresholds)
    return jnp.swapaxes(wavelet_shrink(source, thresholds, image.shape[2]), 1, 2)


def solution(mesh):
    return jax.shard_map(
        shrinkage_step,
        mesh=mesh,
        in_specs=(
            P("groups", None, ("slab", "row"), None),
            P("groups", "coil", None, ("slab", "row"), None),
            P("groups", "coil", ("slab", "row"), None, None),
            P(("slab", "row"), None),
            P(),
        ),
        out_specs=P("groups", None, ("slab", "row"), None),
        check_vma=False,
    )
```

```python
import functools
import math

import jax
import jax.numpy as jnp
import ml_dtypes
import numpy as np
from jax import lax
from jax.experimental import pallas as pl
from jax.experimental.pallas import tpu as pltpu
from jax.sharding import PartitionSpec as P

MESH = pl.DeviceIdType.MESH
step_size = 0.5
CALIBRATION = 8
LATE_COILS = 2


def fourier_table(length, sign):
    index = np.arange(length)
    theta = (index[:, None] * index[None, :] % length) * (2.0 * math.pi / length)
    real = np.cos(theta) / math.sqrt(length)
    imaginary = sign * np.sin(theta) / math.sqrt(length)
    return np.stack([np.stack([real, -imaginary]), np.stack([imaginary, real])])


GUARD = 8


def split_plane(read, write, across, offset):
    cells_y, cells_x = across.shape[2] - GUARD, across.shape[3]
    for t in range(2):
        value = read(t)
        moved = pltpu.roll(value, cells_x - offset, 1)
        for b, part in ((0, value + moved), (1, value - moved)):
            across[b, t, :cells_y, :] = part
            across[b, t, cells_y:, :] = part[:GUARD]
    for b in range(2):
        for t in range(2):
            value = across[b, t, :cells_y, :]
            moved = across[b, t, offset : offset + cells_y, :]
            write(b, t, value + moved)
            write(b + 2, t, value - moved)


def shrink_pair(real, imaginary, limit):
    factor = jnp.maximum(1.0 - limit * lax.rsqrt(real * real + imaginary * imaginary), 0.0)
    return real * factor, imaginary * factor


def wavelet_kernel(levels, planes, limits, descent, result, source, across, kept, moved, carry, source_sem, *bands_of):
    halo = 2**levels - 1
    stop = halo + planes
    cells_y, cells_x = source.shape[2:]
    extent = planes + 2 * halo

    def plane_copy(n):
        return pltpu.make_async_copy(descent.at[:, n], source.at[:, n], source_sem.at[n])

    def fetch(n, _):
        plane_copy(n).start()
        return 0

    lax.fori_loop(0, extent, fetch, 0)
    for level in range(levels):
        offset = 2**level
        bands, finer = bands_of[level], bands_of[level - 1] if level else None

        def split(n, _, offset=offset, bands=bands, finer=finer, reach=2 ** (level - 1) if level else 0):
            if finer is None:
                plane_copy(n).wait()

            def read(t):
                if finer is None:
                    return source[t, n]
                return finer[n, 0, t, :cells_y, :] + finer[n + reach, 0, t, :cells_y, :]

            def write(b, t, value):
                bands[n, b, t, :cells_y, :] = value

            split_plane(read, write, across, offset)
            return 0

        if level:
            extent -= 2 ** (level - 1)
        lax.fori_loop(0, extent, split, 0)
    for level in reversed(range(levels)):
        offset = 2**level
        first = halo - (offset - 1)
        start = first - offset
        bands, last = bands_of[level], level == levels - 1
        scale = (2.0 * 2.0**0.5) ** (level + 1)

        def advance(n, _, level=level, offset=offset, first=first, bands=bands, last=last, scale=scale):
            back = lax.rem(n, offset)
            merged = [[], []]
            for b in range(4):
                near = [bands[n, b, t, :cells_y, :] for t in range(2)]
                far = [bands[n + offset, b, t, :cells_y, :] for t in range(2)]
                high = shrink_pair(near[0] - far[0], near[1] - far[1], limits[level, b + 3] * scale)
                if b:
                    low = shrink_pair(near[0] + far[0], near[1] + far[1], limits[level, b - 1] * scale)
                elif last:
                    low = [near[t] + far[t] for t in range(2)]
                else:
                    low = [bands_of[level + 1][n, 0, t, :cells_y, :] for t in range(2)]
                for t in range(2):
                    merged[t].append(low[t] + high[t] + carry[back, b, t, :cells_y, :])
                    carry[back, b, t, :cells_y, :] = low[t] - high[t]
            for t in range(2):
                for b in range(2):
                    kept[b, t, :cells_y, :] = merged[t][b] + merged[t][b + 2]
                    turned = merged[t][b] - merged[t][b + 2]
                    moved[b, t, GUARD:, :] = turned
                    moved[b, t, :GUARD, :] = turned[cells_y - GUARD :]
            for t in range(2):
                low, high = (kept[b, t, :cells_y, :] + moved[b, t, GUARD - offset : GUARD - offset + cells_y, :] for b in range(2))
                value = (low + high + pltpu.roll(low - high, offset, 1)) * 0.015625
                if level:
                    bands[n, 0, t, :cells_y, :] = value
                else:
                    result[t, pl.ds(jnp.maximum(n - halo, 0), cells_y, stride=planes), :] = value
            return 0

        lax.fori_loop(start, stop, advance, 0)


def wavelet_shrink(source, thresholds, planes):
    levels = thresholds.shape[0]
    halo = 2**levels - 1
    parts, _, cells_y, cells_x = source.shape
    plane = (cells_y + GUARD, cells_x)
    guarded = pltpu.VMEM((2, parts) + plane, jnp.float32)
    whole = pl.BlockSpec(memory_space=pltpu.VMEM)
    return pl.pallas_call(
        functools.partial(wavelet_kernel, levels, planes),
        out_shape=jax.ShapeDtypeStruct((parts, cells_y * planes, cells_x), jnp.float32),
        in_specs=[pl.BlockSpec(memory_space=pltpu.SMEM), pl.BlockSpec(memory_space=pltpu.HBM)],
        out_specs=whole,
        scratch_shapes=[
            pltpu.VMEM(source.shape, jnp.float32),
            guarded,
            guarded,
            guarded,
            pltpu.VMEM((2 ** (levels - 1), 4, parts) + plane, jnp.float32),
            pltpu.SemaphoreType.DMA((planes + 2 * halo,)),
        ]
        + [pltpu.VMEM((planes + 2 * halo, 4, parts) + plane, jnp.float32)] * levels,
        compiler_params=pltpu.CompilerParams(vmem_limit_bytes=60 * 2**20),
        name="wavelet",
    )(thresholds, source)


class Sizes:
    def __init__(self, image, sens, measured, thresholds, shards, coil_groups):
        self.shards, self.coil_groups = shards, coil_groups
        _, self.y, self.planes, self.x = image.shape
        self.z = measured.shape[3]
        self.coils = sens.shape[1]
        self.lines = self.y // shards
        self.part_lines = min(self.lines, 4)
        self.parts = self.lines // self.part_lines
        self.group = min(self.planes, 4)
        self.groups = self.planes // self.group
        self.halo = 2 ** thresholds.shape[0] - 1
        self.late = min(LATE_COILS, self.coils)
        self.early = self.coils - self.late
        first = self.y // 2 - CALIBRATION // 2
        self.calibration = (first, first + CALIBRATION)
        self.skipped = [
            [d for d in range(shards) if self.inside(d, h)] for h in range(self.parts)
        ]

    def inside(self, shard, part):
        start = shard * self.lines + part * self.part_lines
        return self.calibration[0] <= start and start + self.part_lines <= self.calibration[1]

    def is_skipped(self, shard, part):
        found = shard < 0
        for d in self.skipped[part]:
            found = found | (shard == d)
        return found


def tables(sizes):
    n, y, z, planes = sizes.shards, sizes.y, sizes.z, sizes.planes
    phase = fourier_table(y, -1.0)
    phase_rows = phase.reshape(2, 2, y, n, sizes.parts, sizes.part_lines)
    phase_rows = phase_rows.transpose(3, 4, 0, 5, 1, 2).reshape(2 * y, 2 * y)
    inverse = fourier_table(y, 1.0)
    inverse_rows = inverse.transpose(0, 3, 1, 2).reshape(2 * y, 2 * y)
    kept = np.zeros((y,))
    for h in range(sizes.parts):
        for d in sizes.skipped[h]:
            start = d * sizes.lines + h * sizes.part_lines
            kept[start : start + sizes.part_lines] = 1.0
    central = inverse * kept[None, None, :, None]
    central = central.reshape(2, 2, n, sizes.parts, sizes.part_lines, y)
    central = central.transpose(0, 5, 2, 3, 1, 4).reshape(2 * y, 2 * y)
    depth = fourier_table(z, -1.0).transpose(0, 3, 1, 2).reshape(2 * z, 2 * z)
    back = fourier_table(z, 1.0).reshape(2, 2, z, n, sizes.groups, sizes.group)
    back = back.transpose(3, 4, 0, 5, 1, 2).reshape(2 * z, 2 * z)
    readout = fourier_table(sizes.x, 1.0).transpose(1, 2, 0, 3).reshape(2 * sizes.x, 2 * sizes.x)
    found = (phase_rows, central, depth, back, inverse_rows, readout)
    return [jnp.asarray(t.astype(np.float32).astype(ml_dtypes.bfloat16)) for t in found]


def dot(left, right):
    return jnp.dot(left, right, preferred_element_type=jnp.float32)


def gradient_kernel(
    sizes, image, sens, measured, mask, phase, central, depth, back, inverse, readout, source,
    out_f, in_f, out_b, in_b, sens_kept, wide, sampled, sens_slots, measured_slots, totals, edge_out, edge_in,
    sens_sem, measured_sem, out_f_sem, in_f_sem, out_b_sem, in_b_sem, out_q_sem, in_q_sem,
    total_out_sem, total_in_sem, edge_out_sem, edge_in_sem,
):
    n, x = sizes.shards, sizes.x
    coils, early, late = sizes.coils, sizes.early, sizes.late
    planes, halo, pair = sizes.planes, sizes.halo, 2
    rows_f = 2 * sizes.part_lines
    rows_b = 2 * sizes.group
    cells = sizes.y * planes
    rows_n = lax.axis_size("row")
    here = lax.axis_index("slab") * rows_n + lax.axis_index("row")
    scan, coil_here = lax.axis_index("groups"), lax.axis_index("coil")

    def device(shard, coil=None):
        return (scan, shard // rows_n, coil_here if coil is None else coil, lax.rem(shard, rows_n))

    def remote(src, dst, sent, got, target):
        return pltpu.make_async_remote_copy(
            src_ref=src, dst_ref=dst, send_sem=sent, recv_sem=got, device_id=target, device_id_type=MESH
        )

    def arrived(ref, sem):
        pltpu.make_async_copy(ref, ref, sem).wait()

    def sens_copy(c):
        slot = lax.rem(c, 2)
        return pltpu.make_async_copy(sens.at[:, c], sens_slots.at[slot], sens_sem.at[slot])

    def measured_copy(c):
        slot = lax.rem(c, 2)
        return pltpu.make_async_copy(measured.at[:, c], measured_slots.at[slot], measured_sem.at[slot])

    sens_copy(0).start()

    def forward(c, pieces):
        slot = lax.rem(c, 2)

        @pl.when(c + 1 < coils)
        def _():
            sens_copy(c + 1).start()

        sens_copy(c).wait()
        block = cells // 16

        def widen(i, _):
            at = pl.multiple_of(i * block, block)
            for t in range(2):
                wide[pl.ds(t * cells + at, block), :] = sens_slots[slot, t, pl.ds(at, block), :].astype(jnp.float32)
            return 0

        lax.fori_loop(0, 16, widen, 0)

        def plane(p, _):
            sr, si = (wide[pl.ds(t * cells + p, sizes.y, stride=planes), :] for t in range(2))
            ur, ui = (image[t, pl.ds(p, sizes.y, stride=planes), :] for t in range(2))
            sens_kept[c, 0, p] = sr.astype(jnp.bfloat16)
            sens_kept[c, 1, p] = si.astype(jnp.bfloat16)
            coil_image = jnp.concatenate([sr * ur - si * ui, sr * ui + si * ur], axis=0).astype(jnp.bfloat16)
            done = dot(phase[...], coil_image).reshape(n, sizes.parts, rows_f, x)
            out_f[c, :, :, p] = done.astype(jnp.bfloat16)
            return 0

        share = planes // pieces

        def piece(k, _):
            lax.fori_loop(k * share, (k + 1) * share, plane, 0)
            taken = pl.ds(k * share, share)

            def send(d, _):
                to = lax.rem(here + d, n)
                for h in range(sizes.parts):

                    @pl.when(jnp.logical_not(sizes.is_skipped(to, h)))
                    def _():
                        remote(
                            out_f.at[c, to, h, taken], in_f.at[c, here, h, taken],
                            out_f_sem.at[c, h], in_f_sem.at[c, h], device(to),
                        ).start()

                return 0

            lax.fori_loop(1, n, send, 0)
            return 0

        lax.fori_loop(0, pieces, piece, 0)
        for h in range(sizes.parts):
            in_f[c, here, h] = out_f[c, here, h]

        def middle(p, _):
            lines = out_f[c, :, :, p].astype(jnp.float32).reshape(2 * sizes.y, x).astype(jnp.bfloat16)
            value = dot(central[...], lines)
            add_gradient(c, p, value[: sizes.y], value[sizes.y :], c == 0)
            return 0

        lax.fori_loop(0, planes, middle, 0)
        return 0

    def add_gradient(c, p, real, imaginary, fresh=None):
        sr = sens_kept[c, 0, p].astype(jnp.float32)
        si = sens_kept[c, 1, p].astype(jnp.float32)
        for t, term in ((0, sr * real + si * imaginary), (1, sr * imaginary - si * real)):
            held = source[t, halo + p]
            if fresh is not None:
                held = jnp.where(fresh, jnp.zeros_like(held), held)
            source[t, halo + p] = held + term

    forward(jnp.int32(0), math.gcd(planes, 4))
    lax.fori_loop(1, coils, lambda c, _: forward(c, 1), 0)

    measured_copy(0).start()
    kept = mask[...].astype(jnp.float32)
    if sizes.lines % 8:
        kept = jnp.concatenate([kept, jnp.zeros((8 - sizes.lines % 8, sizes.z), jnp.float32)], axis=0)
    kept = kept.T
    for line in range(sizes.lines):
        sampled[line] = jnp.broadcast_to(kept[:, line : line + 1], (sizes.z, x))

    def lines_of(c, _):
        slot = lax.rem(c, 2)

        @pl.when(c + 1 < coils)
        def _():
            measured_copy(c + 1).start()

        measured_copy(c).wait()
        for h in range(sizes.parts):
            skipped = sizes.is_skipped(here, h)

            @pl.when(jnp.logical_not(skipped))
            def _():
                arrived(in_f.at[c, pl.ds(0, n - 1), h], in_f_sem.at[c, h])

                def widen(i, _):
                    rows = planes * rows_f
                    at = pl.multiple_of(i * rows, rows)
                    wide[pl.ds(at, rows), :] = in_f[c, i, h].astype(jnp.float32).reshape(rows, x)
                    return 0

                lax.fori_loop(0, n, widen, 0)

            @pl.when(skipped)
            def _():
                def clear(i, _):
                    rows = planes * rows_f
                    wide[pl.ds(pl.multiple_of(i * rows, rows), rows), :] = jnp.zeros((rows, x), jnp.float32)
                    return 0

                lax.fori_loop(0, n, clear, 0)

            def two_lines(i, _):
                across = []
                for j in range(pair):
                    row = i * pair + j
                    parts = [wide[pl.ds(t * sizes.part_lines + row, sizes.z, stride=rows_f), :] for t in range(2)]
                    across.append(jnp.concatenate(parts, axis=0).astype(jnp.bfloat16))
                spectrum = dot(depth[...], jnp.concatenate(across, axis=1))
                residuals = []
                for j in range(pair):
                    line = h * sizes.part_lines + i * pair + j
                    both = jnp.concatenate([measured_slots[slot, t, line] for t in range(2)], axis=1)
                    data = dot(both, readout[...])
                    keep = sampled[line]
                    columns = slice(j * x, (j + 1) * x)
                    residuals.append(
                        jnp.concatenate(
                            [
                                keep * (spectrum[: sizes.z, columns] - data[:, :x]),
                                keep * (spectrum[sizes.z :, columns] - data[:, x:]),
                            ],
                            axis=0,
                        ).astype(jnp.bfloat16)
                    )
                returned = dot(back[...], jnp.concatenate(residuals, axis=1))
                for j in range(pair):
                    line = h * sizes.part_lines + i * pair + j
                    value = returned[:, j * x : (j + 1) * x].reshape(n, sizes.groups, rows_b, x)
                    out_b[c, :, :, line] = value.astype(jnp.bfloat16)
                return 0

            lax.fori_loop(0, sizes.part_lines // pair, two_lines, 0)

        in_b[c, here] = out_b[c, here]

        @pl.when(c < early)
        def _():
            def send(d, _):
                to = lax.rem(here + d, n)
                remote(out_b.at[c, to], in_b.at[c, here], out_b_sem.at[c], in_b_sem.at[c], device(to)).start()
                return 0

            lax.fori_loop(1, n, send, 0)

        return 0

    lax.fori_loop(0, coils, lines_of, 0)
    order = [0] + ([sizes.groups - 1] if sizes.groups > 1 else []) + list(range(1, sizes.groups - 1))
    last = pl.ds(early, late)
    for q in order:

        def send(d, _, q=q):
            to = lax.rem(here + d, n)
            remote(out_b.at[last, to, q], in_b.at[last, here, q], out_q_sem.at[q], in_q_sem.at[q], device(to)).start()
            return 0

        lax.fori_loop(1, n, send, 0)

    area = sizes.y * rows_b

    def widen_back(c, q, base):
        rows = sizes.lines * rows_b

        def widen(i, _):
            at = pl.multiple_of(base + i * rows, rows)
            wide[pl.ds(at, rows), :] = in_b[c, i, q].astype(jnp.float32).reshape(rows, x)
            return 0

        lax.fori_loop(0, n, widen, 0)

    def two_planes(c, q, i, base):
        across = []
        for j in range(pair):
            row = base + i * pair + j
            parts = [wide[pl.ds(t * sizes.group + row, sizes.y, stride=rows_b), :] for t in range(2)]
            across.append(jnp.concatenate(parts, axis=0).astype(jnp.bfloat16))
        value = dot(inverse[...], jnp.concatenate(across, axis=1))
        for j in range(pair):
            columns = slice(j * x, (j + 1) * x)
            add_gradient(c, q * sizes.group + i * pair + j, value[: sizes.y, columns], value[sizes.y :, columns])

    def early_coil(c, _):
        arrived(in_b.at[c, pl.ds(0, n - 1)], in_b_sem.at[c])

        def each(q, _):
            widen_back(c, q, 0)
            for i in range(sizes.group // pair):
                two_planes(c, q, i, 0)
            return 0

        lax.fori_loop(0, sizes.groups, each, 0)
        return 0

    lax.fori_loop(0, early, early_coil, 0)

    def total_copy(q, i, distance):
        to = lax.rem(coil_here + distance, sizes.coil_groups)
        ref = totals.at[coil_here, q, i]
        return remote(ref, ref, total_out_sem.at[q, i, distance - 1], total_in_sem.at[q, i, distance - 1], device(here, to))

    def late_group(q):
        for c in range(late):
            widen_back(early + c, q, c * area)
        for i in range(sizes.group // pair):
            for c in range(late):
                two_planes(early + c, q, i, c * area)
            for t in range(2):
                for j in range(pair):
                    value = source[t, halo + q * sizes.group + i * pair + j]
                    totals[coil_here, q, i, t, j] = value.astype(jnp.bfloat16)
            for distance in range(1, sizes.coil_groups):
                total_copy(q, i, distance).start()

    def finish(q):
        for i in range(sizes.group // pair):
            for distance in range(1, sizes.coil_groups):
                total_copy(q, i, distance).wait_recv()
            for j in range(pair):
                p = q * sizes.group + i * pair + j
                for t in range(2):
                    total = totals[0, q, i, t, j].astype(jnp.float32)
                    for k in range(1, sizes.coil_groups):
                        total = total + totals[k, q, i, t, j].astype(jnp.float32)
                    source[t, halo + p] = image[t, pl.ds(p, sizes.y, stride=planes), :] - step_size * total

    def edge_copy(side):
        to = lax.rem(here + (1, n - 1)[side], n)
        return remote(edge_out.at[side], edge_in.at[side], edge_out_sem.at[side], edge_in_sem.at[side], device(to))

    ends = set(order[:2])
    for step, q in enumerate(order):
        arrived(in_b.at[last, pl.ds(0, n - 1), q], in_q_sem.at[q])

        late_group(q)
        done = order[:step] if step else []
        if done:
            finish(done[-1])
        if ends.issubset(done) and not ends.issubset(done[:-1]):
            exchange_edges = True
        else:
            exchange_edges = False
        if exchange_edges:
            for t in range(2):
                edge_out[0, t] = source[t, planes : planes + halo].astype(jnp.bfloat16)
                edge_out[1, t] = source[t, halo : 2 * halo].astype(jnp.bfloat16)
            for side in range(2):
                edge_copy(side).start()
    finish(order[-1])
    if not ends.issubset(order[:-1]):
        for t in range(2):
            edge_out[0, t] = source[t, planes : planes + halo].astype(jnp.bfloat16)
            edge_out[1, t] = source[t, halo : 2 * halo].astype(jnp.bfloat16)
        for side in range(2):
            edge_copy(side).start()
    for side in range(2):
        edge_copy(side).wait_recv()
    for t in range(2):
        source[t, :halo] = edge_in[0, t].astype(jnp.float32)
        source[t, halo + planes :] = edge_in[1, t].astype(jnp.float32)

    for side in range(2):
        edge_copy(side).wait_send()
    for q in order:
        arrived(out_b.at[last, pl.ds(0, n - 1), q], out_q_sem.at[q])
        for distance in range(1, sizes.coil_groups):
            for i in range(sizes.group // pair):
                total_copy(q, i, distance).wait_send()

    def left(c, _):
        for h in range(sizes.parts):
            skipped = sizes.is_skipped(here, h)
            others = n - len(sizes.skipped[h])

            @pl.when(skipped)
            def _():
                arrived(out_f.at[c, pl.ds(0, others), h], out_f_sem.at[c, h])

            @pl.when(jnp.logical_not(skipped))
            def _():
                arrived(out_f.at[c, pl.ds(0, others - 1), h], out_f_sem.at[c, h])

        @pl.when(c < early)
        def _():
            arrived(out_b.at[c, pl.ds(0, n - 1)], out_b_sem.at[c])

        return 0

    lax.fori_loop(0, coils, left, 0)


def descent_planes(image, sens, measured, mask, thresholds):
    sizes = Sizes(image, sens, measured, thresholds, lax.axis_size(("slab", "row")), lax.axis_size("coil"))
    n, x, y, planes, coils = sizes.shards, sizes.x, sizes.y, sizes.planes, sizes.coils
    cells = y * planes
    forward = (coils, n, sizes.parts, planes, 2 * sizes.part_lines, x)
    backward = (coils, n, sizes.groups, sizes.lines, 2 * sizes.group, x)
    bf, dma = jnp.bfloat16, pltpu.SemaphoreType.DMA
    rows = max(2 * cells, n * planes * 2 * sizes.part_lines, sizes.late * y * 2 * sizes.group)
    whole, anywhere = pl.BlockSpec(memory_space=pltpu.VMEM), pl.BlockSpec(memory_space=pl.ANY)
    others = max(sizes.coil_groups - 1, 1)
    return pl.pallas_call(
        functools.partial(gradient_kernel, sizes),
        out_shape=jax.ShapeDtypeStruct((2, planes + 2 * sizes.halo, y, x), jnp.float32),
        in_specs=[whole, anywhere, anywhere] + [whole] * 7,
        out_specs=whole,
        scratch_shapes=[
            pltpu.VMEM(forward, bf),
            pltpu.VMEM(forward, bf),
            pltpu.VMEM(backward, bf),
            pltpu.VMEM(backward, bf),
            pltpu.VMEM((coils, 2, planes, y, x), bf),
            pltpu.VMEM((rows, x), jnp.float32),
            pltpu.VMEM((sizes.lines, sizes.z, x), jnp.float32),
            pltpu.VMEM((2, 2, cells, x), bf),
            pltpu.VMEM((2, 2, sizes.lines, sizes.z, x), bf),
            pltpu.VMEM((sizes.coil_groups, sizes.groups, sizes.group // 2, 2, 2, y, x), bf),
            pltpu.VMEM((2, 2, sizes.halo, y, x), bf),
            pltpu.VMEM((2, 2, sizes.halo, y, x), bf),
            dma((2,)),
            dma((2,)),
            dma((coils, sizes.parts)),
            dma((coils, sizes.parts)),
            dma((coils,)),
            dma((coils,)),
            dma((sizes.groups,)),
            dma((sizes.groups,)),
            dma((sizes.groups, sizes.group // 2, others)),
            dma((sizes.groups, sizes.group // 2, others)),
            dma((2,)),
            dma((2,)),
        ],
        compiler_params=pltpu.CompilerParams(has_side_effects=True, vmem_limit_bytes=67043328),
        name="gradient",
    )(image.reshape(2, cells, x), sens.reshape(2, coils, cells, x), measured, mask, *tables(sizes))


def shrinkage_step(image, sens, measured, mask, thresholds):
    source = descent_planes(image, sens, measured, mask, thresholds)
    return wavelet_shrink(source, thresholds, image.shape[2]).reshape(image.shape)


def solution(mesh):
    return jax.shard_map(
        shrinkage_step,
        mesh=mesh,
        in_specs=(
            P("groups", None, ("slab", "row"), None),
            P("groups", "coil", None, ("slab", "row"), None),
            P("groups", "coil", ("slab", "row"), None, None),
            P(("slab", "row"), None),
            P(),
        ),
        out_specs=P("groups", None, ("slab", "row"), None),
        check_vma=False,
    )
```

```python
import functools
import math

import jax
import jax.numpy as jnp
import ml_dtypes
import numpy as np
from jax import lax
from jax.experimental import pallas as pl
from jax.experimental.pallas import tpu as pltpu
from jax.sharding import PartitionSpec as P

MESH = pl.DeviceIdType.MESH
step_size = 0.5
CALIBRATION = 8
LATE_COILS = 2


def fourier_table(length, sign):
    index = np.arange(length)
    theta = (index[:, None] * index[None, :] % length) * (2.0 * math.pi / length)
    real = np.cos(theta) / math.sqrt(length)
    imaginary = sign * np.sin(theta) / math.sqrt(length)
    return np.stack([np.stack([real, -imaginary]), np.stack([imaginary, real])])


GUARD = 8


def split_plane(read, write, across, offset):
    cells_y, cells_x = across.shape[2] - GUARD, across.shape[3]
    for t in range(2):
        value = read(t)
        moved = pltpu.roll(value, cells_x - offset, 1)
        for b, part in ((0, value + moved), (1, value - moved)):
            across[b, t, :cells_y, :] = part
            across[b, t, cells_y:, :] = part[:GUARD]
    for b in range(2):
        for t in range(2):
            value = across[b, t, :cells_y, :]
            moved = across[b, t, offset : offset + cells_y, :]
            write(b, t, value + moved)
            write(b + 2, t, value - moved)


def shrink_pair(real, imaginary, limit):
    factor = jnp.maximum(1.0 - limit * lax.rsqrt(real * real + imaginary * imaginary), 0.0)
    return real * factor, imaginary * factor


def wavelet_kernel(levels, planes, limits, descent, result, source, across, kept, moved, carry, source_sem, *bands_of):
    halo = 2**levels - 1
    stop = halo + planes
    cells_y, cells_x = source.shape[2:]
    extent = planes + 2 * halo

    def plane_copy(n):
        return pltpu.make_async_copy(descent.at[:, n], source.at[:, n], source_sem.at[n])

    def fetch(n, _):
        plane_copy(n).start()
        return 0

    lax.fori_loop(0, extent, fetch, 0)
    for level in range(levels):
        offset = 2**level
        bands, finer = bands_of[level], bands_of[level - 1] if level else None

        def split(n, _, offset=offset, bands=bands, finer=finer, reach=2 ** (level - 1) if level else 0):
            if finer is None:
                plane_copy(n).wait()

            def read(t):
                if finer is None:
                    return source[t, n]
                return finer[n, 0, t, :cells_y, :] + finer[n + reach, 0, t, :cells_y, :]

            def write(b, t, value):
                bands[n, b, t, :cells_y, :] = value

            split_plane(read, write, across, offset)
            return 0

        if level:
            extent -= 2 ** (level - 1)
        lax.fori_loop(0, extent, split, 0, unroll=2)
    for level in reversed(range(levels)):
        offset = 2**level
        first = halo - (offset - 1)
        start = first - offset
        bands, last = bands_of[level], level == levels - 1
        scale = (2.0 * 2.0**0.5) ** (level + 1)

        def advance(n, _, level=level, offset=offset, first=first, bands=bands, last=last, scale=scale):
            back = lax.rem(n, offset)
            merged = [[], []]
            for b in range(4):
                near = [bands[n, b, t, :cells_y, :] for t in range(2)]
                far = [bands[n + offset, b, t, :cells_y, :] for t in range(2)]
                high = shrink_pair(near[0] - far[0], near[1] - far[1], limits[level, b + 3] * scale)
                if b:
                    low = shrink_pair(near[0] + far[0], near[1] + far[1], limits[level, b - 1] * scale)
                elif last:
                    low = [near[t] + far[t] for t in range(2)]
                else:
                    low = [bands_of[level + 1][n, 0, t, :cells_y, :] for t in range(2)]
                for t in range(2):
                    merged[t].append(low[t] + high[t] + carry[back, b, t, :cells_y, :])
                    carry[back, b, t, :cells_y, :] = low[t] - high[t]
            for t in range(2):
                for b in range(2):
                    kept[b, t, :cells_y, :] = merged[t][b] + merged[t][b + 2]
                    turned = merged[t][b] - merged[t][b + 2]
                    moved[b, t, GUARD:, :] = turned
                    moved[b, t, :GUARD, :] = turned[cells_y - GUARD :]
            for t in range(2):
                low, high = (kept[b, t, :cells_y, :] + moved[b, t, GUARD - offset : GUARD - offset + cells_y, :] for b in range(2))
                value = (low + high + pltpu.roll(low - high, offset, 1)) * 0.015625
                if level:
                    bands[n, 0, t, :cells_y, :] = value
                else:
                    result[t, pl.ds(jnp.maximum(n - halo, 0), cells_y, stride=planes), :] = value
            return 0

        lax.fori_loop(start, stop, advance, 0, unroll=2)


def wavelet_shrink(source, thresholds, planes):
    levels = thresholds.shape[0]
    halo = 2**levels - 1
    parts, _, cells_y, cells_x = source.shape
    plane = (cells_y + GUARD, cells_x)
    guarded = pltpu.VMEM((2, parts) + plane, jnp.float32)
    whole = pl.BlockSpec(memory_space=pltpu.VMEM)
    return pl.pallas_call(
        functools.partial(wavelet_kernel, levels, planes),
        out_shape=jax.ShapeDtypeStruct((parts, cells_y * planes, cells_x), jnp.float32),
        in_specs=[pl.BlockSpec(memory_space=pltpu.SMEM), pl.BlockSpec(memory_space=pltpu.HBM)],
        out_specs=whole,
        scratch_shapes=[
            pltpu.VMEM(source.shape, jnp.float32),
            guarded,
            guarded,
            guarded,
            pltpu.VMEM((2 ** (levels - 1), 4, parts) + plane, jnp.float32),
            pltpu.SemaphoreType.DMA((planes + 2 * halo,)),
        ]
        + [pltpu.VMEM((planes + 2 * halo, 4, parts) + plane, jnp.float32)] * levels,
        compiler_params=pltpu.CompilerParams(vmem_limit_bytes=60 * 2**20),
        name="wavelet",
    )(thresholds, source)


class Sizes:
    def __init__(self, image, sens, measured, thresholds, shards, coil_groups):
        self.shards, self.coil_groups = shards, coil_groups
        _, self.y, self.planes, self.x = image.shape
        self.z = measured.shape[3]
        self.coils = sens.shape[1]
        self.lines = self.y // shards
        self.part_lines = min(self.lines, 4)
        self.parts = self.lines // self.part_lines
        self.group = min(self.planes, 4)
        self.groups = self.planes // self.group
        self.halo = 2 ** thresholds.shape[0] - 1
        self.late = min(LATE_COILS, self.coils)
        self.early = self.coils - self.late
        first = self.y // 2 - CALIBRATION // 2
        self.calibration = (first, first + CALIBRATION)
        self.skipped = [
            [d for d in range(shards) if self.inside(d, h)] for h in range(self.parts)
        ]

    def inside(self, shard, part):
        start = shard * self.lines + part * self.part_lines
        return self.calibration[0] <= start and start + self.part_lines <= self.calibration[1]

    def is_skipped(self, shard, part):
        found = shard < 0
        for d in self.skipped[part]:
            found = found | (shard == d)
        return found


def tables(sizes):
    n, y, z, planes = sizes.shards, sizes.y, sizes.z, sizes.planes
    phase = fourier_table(y, -1.0)
    phase_rows = phase.reshape(2, 2, y, n, sizes.parts, sizes.part_lines)
    phase_rows = phase_rows.transpose(3, 4, 0, 5, 1, 2).reshape(2 * y, 2 * y)
    inverse = fourier_table(y, 1.0)
    inverse_rows = inverse.transpose(0, 3, 1, 2).reshape(2 * y, 2 * y)
    kept = np.zeros((y,))
    for h in range(sizes.parts):
        for d in sizes.skipped[h]:
            start = d * sizes.lines + h * sizes.part_lines
            kept[start : start + sizes.part_lines] = 1.0
    central = inverse * kept[None, None, :, None]
    central = central.reshape(2, 2, n, sizes.parts, sizes.part_lines, y)
    central = central.transpose(0, 5, 2, 3, 1, 4).reshape(2 * y, 2 * y)
    depth = fourier_table(z, -1.0).transpose(0, 3, 1, 2).reshape(2 * z, 2 * z)
    back = fourier_table(z, 1.0).reshape(2, 2, z, n, sizes.groups, sizes.group)
    back = back.transpose(3, 4, 0, 5, 1, 2).reshape(2 * z, 2 * z)
    readout = fourier_table(sizes.x, 1.0).transpose(1, 2, 0, 3).reshape(2 * sizes.x, 2 * sizes.x)
    found = (phase_rows, central, depth, back, inverse_rows, readout)
    return [jnp.asarray(t.astype(np.float32).astype(ml_dtypes.bfloat16)) for t in found]


def dot(left, right):
    return jnp.dot(left, right, preferred_element_type=jnp.float32)


def gradient_kernel(
    sizes, image, sens, measured, mask, phase, central, depth, back, inverse, readout, source,
    out_f, in_f, out_b, in_b, sens_kept, wide, sampled, sens_slots, measured_slots, totals, edge_out, edge_in,
    sens_sem, measured_sem, out_f_sem, in_f_sem, out_b_sem, in_b_sem, out_q_sem, in_q_sem,
    total_out_sem, total_in_sem, edge_out_sem, edge_in_sem,
):
    n, x = sizes.shards, sizes.x
    coils, early, late = sizes.coils, sizes.early, sizes.late
    planes, halo, pair = sizes.planes, sizes.halo, 2
    rows_f = 2 * sizes.part_lines
    rows_b = 2 * sizes.group
    cells = sizes.y * planes
    rows_n = lax.axis_size("row")
    here = lax.axis_index("slab") * rows_n + lax.axis_index("row")
    scan, coil_here = lax.axis_index("groups"), lax.axis_index("coil")

    def device(shard, coil=None):
        return (scan, shard // rows_n, coil_here if coil is None else coil, lax.rem(shard, rows_n))

    def remote(src, dst, sent, got, target):
        return pltpu.make_async_remote_copy(
            src_ref=src, dst_ref=dst, send_sem=sent, recv_sem=got, device_id=target, device_id_type=MESH
        )

    def arrived(ref, sem):
        pltpu.make_async_copy(ref, ref, sem).wait()

    def sens_copy(c):
        slot = lax.rem(c, 2)
        return pltpu.make_async_copy(sens.at[:, c], sens_slots.at[slot], sens_sem.at[slot])

    def measured_copy(c):
        slot = lax.rem(c, 2)
        return pltpu.make_async_copy(measured.at[:, c], measured_slots.at[slot], measured_sem.at[slot])

    sens_copy(0).start()

    def forward(c, pieces):
        slot = lax.rem(c, 2)

        @pl.when(c + 1 < coils)
        def _():
            sens_copy(c + 1).start()

        sens_copy(c).wait()
        block = cells // 16

        def widen(i, _):
            at = pl.multiple_of(i * block, block)
            for t in range(2):
                wide[pl.ds(t * cells + at, block), :] = sens_slots[slot, t, pl.ds(at, block), :].astype(jnp.float32)
            return 0

        lax.fori_loop(0, 16, widen, 0)

        def plane(p, _):
            sr, si = (wide[pl.ds(t * cells + p, sizes.y, stride=planes), :] for t in range(2))
            ur, ui = (image[t, pl.ds(p, sizes.y, stride=planes), :] for t in range(2))
            sens_kept[c, 0, p] = sr.astype(jnp.bfloat16)
            sens_kept[c, 1, p] = si.astype(jnp.bfloat16)
            coil_image = jnp.concatenate([sr * ur - si * ui, sr * ui + si * ur], axis=0).astype(jnp.bfloat16)
            done = dot(phase[...], coil_image).reshape(n, sizes.parts, rows_f, x)
            out_f[c, :, :, p] = done.astype(jnp.bfloat16)
            return 0

        share = planes // pieces

        def piece(k, _):
            lax.fori_loop(k * share, (k + 1) * share, plane, 0)
            taken = pl.ds(k * share, share)

            def send(d, _):
                to = lax.rem(here + d, n)
                for h in range(sizes.parts):

                    @pl.when(jnp.logical_not(sizes.is_skipped(to, h)))
                    def _():
                        remote(
                            out_f.at[c, to, h, taken], in_f.at[c, here, h, taken],
                            out_f_sem.at[c, h], in_f_sem.at[c, h], device(to),
                        ).start()

                return 0

            lax.fori_loop(1, n, send, 0)
            return 0

        lax.fori_loop(0, pieces, piece, 0)
        for h in range(sizes.parts):
            in_f[c, here, h] = out_f[c, here, h]

        def middle(p, _):
            lines = out_f[c, :, :, p].astype(jnp.float32).reshape(2 * sizes.y, x).astype(jnp.bfloat16)
            value = dot(central[...], lines)
            add_gradient(c, p, value[: sizes.y], value[sizes.y :], c == 0)
            return 0

        lax.fori_loop(0, planes, middle, 0)
        return 0

    def add_gradient(c, p, real, imaginary, fresh=None):
        sr = sens_kept[c, 0, p].astype(jnp.float32)
        si = sens_kept[c, 1, p].astype(jnp.float32)
        for t, term in ((0, sr * real + si * imaginary), (1, sr * imaginary - si * real)):
            held = source[t, halo + p]
            if fresh is not None:
                held = jnp.where(fresh, jnp.zeros_like(held), held)
            source[t, halo + p] = held + term

    forward(jnp.int32(0), math.gcd(planes, 4))
    lax.fori_loop(1, coils, lambda c, _: forward(c, 1), 0)

    measured_copy(0).start()
    kept = mask[...].astype(jnp.float32)
    if sizes.lines % 8:
        kept = jnp.concatenate([kept, jnp.zeros((8 - sizes.lines % 8, sizes.z), jnp.float32)], axis=0)
    kept = kept.T
    for line in range(sizes.lines):
        sampled[line] = jnp.broadcast_to(kept[:, line : line + 1], (sizes.z, x))

    def lines_of(c, _):
        slot = lax.rem(c, 2)

        @pl.when(c + 1 < coils)
        def _():
            measured_copy(c + 1).start()

        measured_copy(c).wait()
        for h in range(sizes.parts):
            skipped = sizes.is_skipped(here, h)

            @pl.when(jnp.logical_not(skipped))
            def _():
                arrived(in_f.at[c, pl.ds(0, n - 1), h], in_f_sem.at[c, h])

                def widen(i, _):
                    rows = planes * rows_f
                    at = pl.multiple_of(i * rows, rows)
                    wide[pl.ds(at, rows), :] = in_f[c, i, h].astype(jnp.float32).reshape(rows, x)
                    return 0

                lax.fori_loop(0, n, widen, 0)

            @pl.when(skipped)
            def _():
                def clear(i, _):
                    rows = planes * rows_f
                    wide[pl.ds(pl.multiple_of(i * rows, rows), rows), :] = jnp.zeros((rows, x), jnp.float32)
                    return 0

                lax.fori_loop(0, n, clear, 0)

            def two_lines(i, _):
                across = []
                for j in range(pair):
                    row = i * pair + j
                    parts = [wide[pl.ds(t * sizes.part_lines + row, sizes.z, stride=rows_f), :] for t in range(2)]
                    across.append(jnp.concatenate(parts, axis=0).astype(jnp.bfloat16))
                spectrum = dot(depth[...], jnp.concatenate(across, axis=1))
                residuals = []
                for j in range(pair):
                    line = h * sizes.part_lines + i * pair + j
                    both = jnp.concatenate([measured_slots[slot, t, line] for t in range(2)], axis=1)
                    data = dot(both, readout[...])
                    keep = sampled[line]
                    columns = slice(j * x, (j + 1) * x)
                    residuals.append(
                        jnp.concatenate(
                            [
                                keep * (spectrum[: sizes.z, columns] - data[:, :x]),
                                keep * (spectrum[sizes.z :, columns] - data[:, x:]),
                            ],
                            axis=0,
                        ).astype(jnp.bfloat16)
                    )
                returned = dot(back[...], jnp.concatenate(residuals, axis=1))
                for j in range(pair):
                    line = h * sizes.part_lines + i * pair + j
                    value = returned[:, j * x : (j + 1) * x].reshape(n, sizes.groups, rows_b, x)
                    out_b[c, :, :, line] = value.astype(jnp.bfloat16)
                return 0

            lax.fori_loop(0, sizes.part_lines // pair, two_lines, 0)

        in_b[c, here] = out_b[c, here]

        @pl.when(c < early)
        def _():
            def send(d, _):
                to = lax.rem(here + d, n)
                remote(out_b.at[c, to], in_b.at[c, here], out_b_sem.at[c], in_b_sem.at[c], device(to)).start()
                return 0

            lax.fori_loop(1, n, send, 0)

        return 0

    lax.fori_loop(0, coils, lines_of, 0)
    order = [0] + ([sizes.groups - 1] if sizes.groups > 1 else []) + list(range(1, sizes.groups - 1))
    last = pl.ds(early, late)
    for q in order:

        def send(d, _, q=q):
            to = lax.rem(here + d, n)
            remote(out_b.at[last, to, q], in_b.at[last, here, q], out_q_sem.at[q], in_q_sem.at[q], device(to)).start()
            return 0

        lax.fori_loop(1, n, send, 0)

    area = sizes.y * rows_b

    def widen_back(c, q, base):
        rows = sizes.lines * rows_b

        def widen(i, _):
            at = pl.multiple_of(base + i * rows, rows)
            wide[pl.ds(at, rows), :] = in_b[c, i, q].astype(jnp.float32).reshape(rows, x)
            return 0

        lax.fori_loop(0, n, widen, 0)

    def two_planes(c, q, i, base):
        across = []
        for j in range(pair):
            row = base + i * pair + j
            parts = [wide[pl.ds(t * sizes.group + row, sizes.y, stride=rows_b), :] for t in range(2)]
            across.append(jnp.concatenate(parts, axis=0).astype(jnp.bfloat16))
        value = dot(inverse[...], jnp.concatenate(across, axis=1))
        for j in range(pair):
            columns = slice(j * x, (j + 1) * x)
            add_gradient(c, q * sizes.group + i * pair + j, value[: sizes.y, columns], value[sizes.y :, columns])

    def early_coil(c, _):
        arrived(in_b.at[c, pl.ds(0, n - 1)], in_b_sem.at[c])

        def each(q, _):
            widen_back(c, q, 0)
            for i in range(sizes.group // pair):
                two_planes(c, q, i, 0)
            return 0

        lax.fori_loop(0, sizes.groups, each, 0)
        return 0

    lax.fori_loop(0, early, early_coil, 0)

    def total_copy(q, i, distance):
        to = lax.rem(coil_here + distance, sizes.coil_groups)
        ref = totals.at[coil_here, q, i]
        return remote(ref, ref, total_out_sem.at[q, i, distance - 1], total_in_sem.at[q, i, distance - 1], device(here, to))

    def late_group(q):
        for c in range(late):
            widen_back(early + c, q, c * area)
        for i in range(sizes.group // pair):
            for c in range(late):
                two_planes(early + c, q, i, c * area)
            for t in range(2):
                for j in range(pair):
                    value = source[t, halo + q * sizes.group + i * pair + j]
                    totals[coil_here, q, i, t, j] = value.astype(jnp.bfloat16)
            for distance in range(1, sizes.coil_groups):
                total_copy(q, i, distance).start()

    def finish(q):
        for i in range(sizes.group // pair):
            for distance in range(1, sizes.coil_groups):
                total_copy(q, i, distance).wait_recv()
            for j in range(pair):
                p = q * sizes.group + i * pair + j
                for t in range(2):
                    total = totals[0, q, i, t, j].astype(jnp.float32)
                    for k in range(1, sizes.coil_groups):
                        total = total + totals[k, q, i, t, j].astype(jnp.float32)
                    source[t, halo + p] = image[t, pl.ds(p, sizes.y, stride=planes), :] - step_size * total

    def edge_copy(side):
        to = lax.rem(here + (1, n - 1)[side], n)
        return remote(edge_out.at[side], edge_in.at[side], edge_out_sem.at[side], edge_in_sem.at[side], device(to))

    ends = set(order[:2])
    for step, q in enumerate(order):
        arrived(in_b.at[last, pl.ds(0, n - 1), q], in_q_sem.at[q])

        late_group(q)
        done = order[:step] if step else []
        if done:
            finish(done[-1])
        if ends.issubset(done) and not ends.issubset(done[:-1]):
            exchange_edges = True
        else:
            exchange_edges = False
        if exchange_edges:
            for t in range(2):
                edge_out[0, t] = source[t, planes : planes + halo].astype(jnp.bfloat16)
                edge_out[1, t] = source[t, halo : 2 * halo].astype(jnp.bfloat16)
            for side in range(2):
                edge_copy(side).start()
    finish(order[-1])
    if not ends.issubset(order[:-1]):
        for t in range(2):
            edge_out[0, t] = source[t, planes : planes + halo].astype(jnp.bfloat16)
            edge_out[1, t] = source[t, halo : 2 * halo].astype(jnp.bfloat16)
        for side in range(2):
            edge_copy(side).start()
    for side in range(2):
        edge_copy(side).wait_recv()
    for t in range(2):
        source[t, :halo] = edge_in[0, t].astype(jnp.float32)
        source[t, halo + planes :] = edge_in[1, t].astype(jnp.float32)

    for side in range(2):
        edge_copy(side).wait_send()
    for q in order:
        arrived(out_b.at[last, pl.ds(0, n - 1), q], out_q_sem.at[q])
        for distance in range(1, sizes.coil_groups):
            for i in range(sizes.group // pair):
                total_copy(q, i, distance).wait_send()

    def left(c, _):
        for h in range(sizes.parts):
            skipped = sizes.is_skipped(here, h)
            others = n - len(sizes.skipped[h])

            @pl.when(skipped)
            def _():
                arrived(out_f.at[c, pl.ds(0, others), h], out_f_sem.at[c, h])

            @pl.when(jnp.logical_not(skipped))
            def _():
                arrived(out_f.at[c, pl.ds(0, others - 1), h], out_f_sem.at[c, h])

        @pl.when(c < early)
        def _():
            arrived(out_b.at[c, pl.ds(0, n - 1)], out_b_sem.at[c])

        return 0

    lax.fori_loop(0, coils, left, 0)


def descent_planes(image, sens, measured, mask, thresholds):
    sizes = Sizes(image, sens, measured, thresholds, lax.axis_size(("slab", "row")), lax.axis_size("coil"))
    n, x, y, planes, coils = sizes.shards, sizes.x, sizes.y, sizes.planes, sizes.coils
    cells = y * planes
    forward = (coils, n, sizes.parts, planes, 2 * sizes.part_lines, x)
    backward = (coils, n, sizes.groups, sizes.lines, 2 * sizes.group, x)
    bf, dma = jnp.bfloat16, pltpu.SemaphoreType.DMA
    rows = max(2 * cells, n * planes * 2 * sizes.part_lines, sizes.late * y * 2 * sizes.group)
    whole, anywhere = pl.BlockSpec(memory_space=pltpu.VMEM), pl.BlockSpec(memory_space=pl.ANY)
    others = max(sizes.coil_groups - 1, 1)
    return pl.pallas_call(
        functools.partial(gradient_kernel, sizes),
        out_shape=jax.ShapeDtypeStruct((2, planes + 2 * sizes.halo, y, x), jnp.float32),
        in_specs=[whole, anywhere, anywhere] + [whole] * 7,
        out_specs=whole,
        scratch_shapes=[
            pltpu.VMEM(forward, bf),
            pltpu.VMEM(forward, bf),
            pltpu.VMEM(backward, bf),
            pltpu.VMEM(backward, bf),
            pltpu.VMEM((coils, 2, planes, y, x), bf),
            pltpu.VMEM((rows, x), jnp.float32),
            pltpu.VMEM((sizes.lines, sizes.z, x), jnp.float32),
            pltpu.VMEM((2, 2, cells, x), bf),
            pltpu.VMEM((2, 2, sizes.lines, sizes.z, x), bf),
            pltpu.VMEM((sizes.coil_groups, sizes.groups, sizes.group // 2, 2, 2, y, x), bf),
            pltpu.VMEM((2, 2, sizes.halo, y, x), bf),
            pltpu.VMEM((2, 2, sizes.halo, y, x), bf),
            dma((2,)),
            dma((2,)),
            dma((coils, sizes.parts)),
            dma((coils, sizes.parts)),
            dma((coils,)),
            dma((coils,)),
            dma((sizes.groups,)),
            dma((sizes.groups,)),
            dma((sizes.groups, sizes.group // 2, others)),
            dma((sizes.groups, sizes.group // 2, others)),
            dma((2,)),
            dma((2,)),
        ],
        compiler_params=pltpu.CompilerParams(has_side_effects=True, vmem_limit_bytes=67043328),
        name="gradient",
    )(image.reshape(2, cells, x), sens.reshape(2, coils, cells, x), measured, mask, *tables(sizes))


def shrinkage_step(image, sens, measured, mask, thresholds):
    source = descent_planes(image, sens, measured, mask, thresholds)
    return wavelet_shrink(source, thresholds, image.shape[2]).reshape(image.shape)


def solution(mesh):
    return jax.shard_map(
        shrinkage_step,
        mesh=mesh,
        in_specs=(
            P("groups", None, ("slab", "row"), None),
            P("groups", "coil", None, ("slab", "row"), None),
            P("groups", "coil", ("slab", "row"), None, None),
            P(("slab", "row"), None),
            P(),
        ),
        out_specs=P("groups", None, ("slab", "row"), None),
        check_vma=False,
    )
```
